32 devices in a mesh: rows: 4 (over y, x), feat: 8 (over z, core).
Axes of the slice: x: 2, y: 2, z: 4, core: 2. Of those that a mesh axis runs over, the one named last changes fastest.
Arguments:
- bins: int32 [768, 16384], P('feat', 'rows'), may hold values from 0 to 255
- fold: int32 [16384], P('rows'), may hold values from 0 to 9
- nodes: int32 [16384, 10], P('rows'), may hold values from 0 to 3
- gradient: bfloat16 [16384], P('rows'), may hold values from -6 to 6
- hessian: bfloat16 [16384], P('rows'), may hold values from 0.049804688 to 1
Outputs:
- train_hist: float32 [80, 768, 256], P('rows', 'feat')
- node_gain: float32 [10, 4], replicated
The draws below stay inside these ranges and needn't reach their ends.
All inputs are finite; a program needn't handle non-finite values.
Results may differ from the reference program's by a relative error of at most 0.0003.
Values sent between devices are 32-bit elements; how exact they have to be, the bound alone decides.
No kernel may reach another device: no remote copies, remote signals or barrier semaphores. Data moves between devices by JAX's collectives and lax.ppermute only.
A program may use at most 64 MiB of HBM per device.

```python
import math
import jax
import jax.numpy as jnp
from jax import lax

F = 768
BINS = 256
FOLDS = 10
NODES = 4
ROWS = 16384


def with_ends(entries, own_key, low, top_value):
    longest = entries.shape.index(max(entries.shape))
    spots = []
    for shift in (0, 1):
        where = [jax.random.randint(jax.random.fold_in(own_key, axis), (), 0, length) for axis, length in enumerate(entries.shape)]
        where[longest] = (where[longest] + shift) % entries.shape[longest]
        spots.append(tuple(where))
    return entries.at[spots[0]].set(low).at[spots[1]].set(top_value)


def block_scale(stream_key, dims, shards, smallest, high):
    loudness, own = 1.0, jax.random.fold_in(stream_key, 6)
    for axis_at, shards_of in shards:
        steps = jnp.exp(jax.random.uniform(jax.random.fold_in(own, axis_at), (shards_of,), jnp.float32, smallest / len(shards), high / len(shards)))
        loudness = loudness * jnp.repeat(steps, dims[axis_at] // shards_of).reshape([-1 if axis == axis_at else 1 for axis in range(len(dims))])
    return loudness


def bell_draw(own_key, shape, scale, bound, split=(), held_as=jnp.bfloat16):
    values = scale * jax.random.normal(own_key, shape, jnp.float32)
    if split:
        values = values * block_scale(own_key, shape, split, -0.22, 0.18)
    return jnp.clip(values, -bound, bound).astype(held_as)


def setup_inputs(seed: int = 0) -> dict:
    streams_of = jax.random.split(jax.random.key(seed), 6)
    return {
        "bins": with_ends(jax.random.randint(streams_of[0], (F, ROWS), 0, BINS), jax.random.fold_in(streams_of[0], 1), 0, BINS - 1).astype(jnp.int32),
        "fold": with_ends(jax.random.randint(streams_of[1], (ROWS,), 0, FOLDS), jax.random.fold_in(streams_of[1], 1), 0, FOLDS - 1).astype(jnp.int32),
        "nodes": with_ends(jax.random.randint(streams_of[2], (ROWS, FOLDS), 0, NODES), jax.random.fold_in(streams_of[2], 1), 0, NODES - 1).astype(jnp.int32),
        "gradient": bell_draw(streams_of[3], (ROWS,), 1.0, 6.0, ((0, 4),)),
        "hessian": jnp.clip(jnp.exp(math.log(1.0) - 2.9996462 * jax.random.uniform(streams_of[4], (ROWS,), jnp.float32) ** block_scale(streams_of[4], (ROWS,), ((0, 4),), -0.2, 0.2)), 0.049804688, 1.0).astype(jnp.bfloat16),
    }


def reference(bins, fold, nodes, gradient, hessian):
    count = bins.shape[1]
    grad = gradient.astype(jnp.float32)[:, None]
    hess = hessian.astype(jnp.float32)[:, None]
    kept = (fold[:, None] != jnp.arange(FOLDS, dtype=jnp.int32)[None, :])[:, :, None]
    node_hot = nodes[:, :, None] == jnp.arange(NODES, dtype=jnp.int32)[None, None, :]
    selected = (node_hot & kept).reshape(count, FOLDS * NODES).astype(jnp.float32)
    weights = jnp.stack([grad * selected, hess * selected], axis=2).reshape(count, FOLDS * NODES * 2)

    def one_feature(column):
        return jax.ops.segment_sum(weights, column.astype(jnp.int32), num_segments=BINS)

    hist = lax.map(one_feature, bins)
    train_hist = hist.transpose(2, 0, 1)
    paired = train_hist.reshape(FOLDS, NODES, 2, F, BINS)
    totals = jnp.sum(paired[:, :, :, 0, :], axis=-1)
    left = jnp.cumsum(paired, axis=-1)[..., :BINS - 1]
    left_g, left_h = left[:, :, 0], left[:, :, 1]
    whole_g = totals[:, :, 0][:, :, None, None]
    whole_h = totals[:, :, 1][:, :, None, None]
    gain = left_g * left_g / (left_h + 1.0) + (whole_g - left_g) ** 2 / (whole_h - left_h + 1.0) - whole_g * whole_g / (whole_h + 1.0)
    node_gain = jnp.max(gain, axis=(2, 3))
    return train_hist, node_gain
```

```python
import functools

import jax
import jax.numpy as jnp
from jax import lax
from jax.experimental import pallas as pl
from jax.experimental.pallas import tpu as pltpu
from jax.sharding import PartitionSpec as P


BINS = 256
FOLDS = 10
NODES = 4
PAIRS = FOLDS * NODES
COLS = 2 * PAIRS
TILE = 256
F8 = jnp.float8_e4m3fn
F32 = jnp.float32
BF16 = jnp.bfloat16


VMEM = pl.BlockSpec(memory_space=pltpu.VMEM)
SMEM = pl.BlockSpec(memory_space=pltpu.SMEM)
ANY = pl.BlockSpec(memory_space=pl.ANY)


def params():
    return pltpu.CompilerParams(vmem_limit_bytes=16 * 2**20)


def cost(flops, bytes_accessed=1 << 20):
    return pl.CostEstimate(
        flops=int(flops), bytes_accessed=int(bytes_accessed), transcendentals=0
    )


def weight_lines(low, high):
    shape = low.shape
    line = lax.broadcasted_iota(jnp.int32, shape, 0)
    node = (line % NODES).astype(F32)
    first = line < NODES
    fold = high[2:3]
    grads, hesss = [], []
    for j in range(FOLDS // 2):
        source, at = (low, 2 * j) if j < 4 else (high, 0)
        placed = jnp.where(first, source[at : at + 1], source[at + 1 : at + 2])
        k = jnp.where(first, F32(2 * j), F32(2 * j + 1))
        chosen = (placed == node) & (fold != k)
        grads.append(jnp.where(chosen, high[3:4], F32(0)))
        hesss.append(jnp.where(chosen, high[4:5], F32(0)))
    return jnp.concatenate(grads + hesss, axis=0).astype(BF16)


def one_hot(row, levels):
    packed = jnp.broadcast_to(row, (16, TILE)).astype(BF16)
    hit = jnp.concatenate([packed] * (BINS // 16), axis=0) == levels
    return jnp.where(hit, jnp.ones((), F8), jnp.zeros((), F8))


def bin_levels():
    return lax.broadcasted_iota(jnp.int32, (BINS, TILE), 0).astype(BF16)


def accumulate_pair(accs, feature, sources, levels):
    turn = 0
    for bins, line, weights, column, rows in sources:
        for at in range(0, rows, TILE):
            lhs = weights[:, pl.ds(column + at, TILE)]
            for q, acc in enumerate(accs):
                row = bins[pl.ds(line + feature + q, 1), pl.ds(at, TILE)]
                pltpu.matmul_push_rhs(
                    one_hot(row, levels), staging_register=turn % 2, mxu_index=q, transpose=True
                )
                pltpu.matmul_acc_lhs(acc, lhs, load_staged_rhs=turn % 2)
            turn += 1


def prepare_kernel(group, owned, size, me, parity, bins, nodes, fold, gradient, hessian, *refs):
    first, later = refs[: group - 1], refs[group - 1 : -2]
    own, rowdata = refs[-2:]
    rows = bins.shape[1]
    rowdata[0:FOLDS] = nodes[...].astype(F32)
    rowdata[FOLDS + 3 :] = jnp.zeros((16 - FOLDS - 3, rows), F32)
    for i, ref in enumerate((fold, gradient, hessian)):
        lines = ref[...].astype(F32)
        for j in range(rows // 128):
            rowdata[FOLDS + i : FOLDS + i + 1, j * 128 : j * 128 + 128] = lines[j : j + 1]

    def move(to, at, source, count):
        if owned % 8 == 0:
            to[at : at + count] = bins[pl.ds(pl.multiple_of(source, 8), count)].astype(F32)
        else:
            for i in range(count):
                to[at + i : at + i + 1] = bins[pl.ds(source + i, 1)].astype(F32)

    for d in range(1, group):
        base = (me[0] ^ d) * owned
        first[d - 1][0:8] = rowdata[pl.ds(pl.multiple_of(parity[0] * 8, 8), 8)]
        move(first[d - 1], 8, base, size)
        if later:
            move(later[d - 1], 0, base + size, owned - size)
    move(own, 0, me[0] * owned, owned)


def prepare(me, parity, bins, nodes, fold, gradient, hessian, group, owned, size):
    rows = bins.shape[1]
    shapes = [(size + 8, rows)] * (group - 1)
    if owned > size:
        shapes += [(owned - size, rows)] * (group - 1)
    shapes += [(owned, rows), (16, rows)]
    wide = (rows // 128, 128)
    out = pl.pallas_call(
        functools.partial(prepare_kernel, group, owned, size),
        out_shape=[jax.ShapeDtypeStruct(shape, F32) for shape in shapes],
        in_specs=[SMEM, SMEM] + [VMEM] * 5,
        out_specs=[VMEM] * len(shapes),
        compiler_params=params(),
        cost_estimate=cost(1 << 30),
        name="prepare",
    )(me, parity, bins, nodes.T, fold.reshape(wide), gradient.reshape(wide), hessian.reshape(wide))
    return out[: group - 1], out[group - 1 : -2], out[-2], out[-1]


def own_kernel(bins, rowdata, *refs):
    outs, weights = refs[:-1], refs[-1]
    feats, rows = bins.shape
    size = feats // len(outs)

    def prepare(i, carry):
        at = pl.ds(pl.multiple_of(i * 512, 512), 512)
        weights[:, at] = weight_lines(rowdata[0:8, at], rowdata[8:16, at])
        return carry

    lax.fori_loop(0, rows // 512, prepare, 0)
    levels = bin_levels()

    def body(acc0, acc1):
        for c, out in enumerate(outs):

            def visit(p, carry, c=c, out=out):
                accumulate_pair((acc0, acc1), 2 * p, [(bins, c * size, weights, 0, rows)], levels)
                for q, acc in enumerate((acc0, acc1)):
                    at = pl.ds(pl.multiple_of((2 * p + q) * COLS, COLS), COLS)
                    out[at] = pltpu.matmul_pop(acc)
                return carry

            lax.fori_loop(0, size // 2, visit, 0)

    pl.run_scoped(body, pltpu.ACC(0)((COLS, BINS), F32), pltpu.ACC(1)((COLS, BINS), F32))


def own_part(bins, rowdata, size):
    feats, rows = bins.shape
    out = jax.ShapeDtypeStruct((size * COLS, BINS), F32)
    return pl.pallas_call(
        own_kernel,
        out_shape=[out] * (feats // size),
        in_specs=[VMEM, VMEM],
        out_specs=[VMEM] * (feats // size),
        scratch_shapes=[pltpu.VMEM((COLS, rows), BF16)],
        compiler_params=params(),
        cost_estimate=cost(2 * feats * rows * COLS * BINS),
        name="own_part",
    )(bins, rowdata)


def weights_kernel(count, rows, parity, *refs):
    mine, other, out = refs[:count], refs[count], refs[count + 1]
    even = parity[0] == 0
    for s in range(count):

        def prepare(i, carry, s=s):
            at = pl.ds(pl.multiple_of(i * 512, 512), 512)
            a = mine[s][0:8, at]
            b = other[8 * s : 8 * s + 8, at]
            to = pl.ds(pl.multiple_of(s * rows + i * 512, 512), 512)
            out[:, to] = weight_lines(jnp.where(even, a, b), jnp.where(even, b, a))
            return carry

        lax.fori_loop(0, rows // 512, prepare, 0)


def remote_weights(parity, mine, other):
    count = len(mine)
    rows = other.shape[1]
    return pl.pallas_call(
        functools.partial(weights_kernel, count, rows),
        out_shape=jax.ShapeDtypeStruct((COLS, count * rows), BF16),
        in_specs=[SMEM] + [VMEM] * (count + 1),
        out_specs=VMEM,
        compiler_params=params(),
        cost_estimate=cost(1 << 30),
        name="remote_weights",
    )(parity, *mine, other)


def chunk_kernel(count, group, line, feats, rows, final, me, part, best_in, weights, *refs):
    bins, pieces, best_out, held = refs[:count], refs[count:-2], refs[-2], refs[-1]
    levels = bin_levels()
    lower = lax.broadcasted_iota(jnp.int32, (BINS, BINS), 0)
    upper = lax.broadcasted_iota(jnp.int32, (BINS, BINS), 1)
    triangle = (lower <= upper).astype(BF16)
    last = lax.broadcasted_iota(jnp.int32, (PAIRS, BINS), 1) == BINS - 1
    sources = [(bins[s], line, weights, s * rows, rows) for s in range(count)]

    def body(acc0, acc1):
        accs = (acc0, acc1)

        def visit(p, carry):
            accumulate_pair(accs, 2 * p, sources, levels)
            for q, acc in enumerate(accs):
                at = pl.ds(pl.multiple_of((2 * p + q) * COLS, COLS), COLS)
                whole = pltpu.matmul_pop(acc) + part[at]
                for half in range(2):
                    held[half, at] = whole[:, half * 128 : half * 128 + 128]
            return carry

        lax.fori_loop(0, feats // 2, visit, 0)

        best = best_in[...]
        for p in range(feats // 2):
            for q, acc in enumerate(accs):
                f = 2 * p + q
                if p == 0:
                    pltpu.matmul_push_rhs(triangle, staging_register=0, mxu_index=q)
                at = slice(f * COLS, (f + 1) * COLS)
                rest = jnp.concatenate([held[0, at], held[1, at]], axis=1)
                for piece in range(3):
                    high = rest.astype(BF16)
                    rest = rest - high.astype(F32)
                    pltpu.matmul_acc_lhs(
                        acc, high, load_staged_rhs=0 if p == 0 and piece == 0 else None
                    )
            for acc in accs:
                left = pltpu.matmul_pop(acc)
                gl, hl = left[:PAIRS], left[PAIRS:]
                g, h = gl[:, BINS - 1 :], hl[:, BINS - 1 :]
                gain = (
                    gl * gl / (hl + 1.0)
                    + (g - gl) * (g - gl) / (h - hl + 1.0)
                    - g * g / (h + 1.0)
                )
                best = jnp.maximum(best, jnp.where(last, F32(-3e38), gain))
        if final:
            best = jnp.broadcast_to(jnp.max(best, axis=1, keepdims=True), (PAIRS, 128))
        best_out[...] = best

    pl.run_scoped(body, pltpu.ACC(0)((COLS, BINS), F32), pltpu.ACC(1)((COLS, BINS), F32))

    share = COLS // group
    for d in range(group):
        for j in range(share):
            row = (j % 2) * PAIRS + (me[0] ^ d) * (share // 2) + j // 2
            for half in range(2):
                pieces[d][j, :, half * 128 : half * 128 + 128] = held[
                    half, pl.ds(row, feats, stride=COLS), :
                ]


def chunk(me, part, best, weights, bins, line, feats, group, final):
    count = len(bins)
    rows = weights.shape[1] // count
    share = COLS // group
    piece = jax.ShapeDtypeStruct((share, feats, BINS), F32)
    out = pl.pallas_call(
        functools.partial(chunk_kernel, count, group, line, feats, rows, final),
        out_shape=[piece] * group + [jax.ShapeDtypeStruct((PAIRS, 128 if final else BINS), F32)],
        in_specs=[SMEM, VMEM, VMEM, VMEM] + [VMEM] * count,
        out_specs=[VMEM] * (group + 1),
        scratch_shapes=[pltpu.VMEM((2, feats * COLS, 128), F32)],
        compiler_params=params(),
        cost_estimate=cost(2 * feats * rows * count * COLS * BINS),
        name="chunk",
    )(me, part, best, weights, *bins)
    return out[:-1], out[-1]


def place_kernel(group, first, owned, feats, me, *refs):
    pieces, out, sems = refs[:group], refs[-2], refs[-1]
    copies = []
    for d in range(group):
        at = pl.multiple_of((me[0] ^ d) * owned + first, 8)
        copies.append(
            pltpu.make_async_copy(pieces[d], out.at[:, pl.ds(at, feats), :], sems.at[d])
        )
    for copy in copies:
        copy.start()
    for copy in copies:
        copy.wait()


def place(me, held, pieces, first, owned, shape):
    group = len(pieces)
    feats = pieces[0].shape[1]
    if owned % 8 or first % 8 or feats % 8:
        if held is None:
            held = jnp.zeros(shape, F32)
        for d, piece in enumerate(pieces):
            held = lax.dynamic_update_slice_in_dim(held, piece, (me[0] ^ d) * owned + first, 1)
        return held
    return pl.pallas_call(
        functools.partial(place_kernel, group, first, owned, feats),
        out_shape=jax.ShapeDtypeStruct(shape, F32),
        in_specs=[SMEM] + [VMEM] * group + ([] if held is None else [ANY]),
        out_specs=ANY,
        scratch_shapes=[pltpu.SemaphoreType.DMA((group,))],
        input_output_aliases={} if held is None else {group + 1: 0},
        compiler_params=params(),
        name="place",
    )(me, *pieces, *([] if held is None else [held]))


def on_device(group, feat_size, bins, fold, nodes, gradient, hessian):
    feats, _ = bins.shape
    owned = feats // group
    size = 8 if owned % 8 == 0 else owned
    chunks = owned // size
    me = lax.axis_index("rows")[None]
    parity = (lax.axis_index("feat") & 1)[None]
    others = range(1, group)

    def swap(x, axis, count, d):
        return lax.ppermute(x, axis, [(i, i ^ d) for i in range(count)])

    first, later, own, rowdata = prepare(
        me, parity, bins, nodes, fold, gradient, hessian, group, owned, size
    )
    arrived = [swap(first[d - 1], "rows", group, d) for d in others]
    if later:
        later = [swap(later[d - 1], "rows", group, d) for d in others]
    part = own_part(own, rowdata, size)
    traded = swap(jnp.concatenate([a[:8] for a in arrived]), "feat", feat_size, 1)
    weights = remote_weights(parity, arrived, traded)
    best = jnp.full((PAIRS, BINS), -3e38, F32)
    received = []
    for c in range(chunks):
        left = chunks - 1 - c
        source, line = (arrived, 8) if c == 0 else (later, (c - 1) * size)
        pieces, best = chunk(
            me, part[c], best, weights, source, line, size, group, left == 0
        )
        received.append([pieces[0]] + [swap(pieces[d], "rows", group, d) for d in others])
    step = 1
    while step < feat_size:
        best = jnp.maximum(best, swap(best, "feat", feat_size, step))
        step *= 2
    tops = [swap(best, "rows", group, d) for d in others]
    out = None
    for c, pieces in enumerate(received):
        out = place(me, out, pieces, c * size, owned, (COLS // group, feats, BINS))
    for top in tops:
        best = jnp.maximum(best, top)
    return out, best[:, 0].reshape(FOLDS, NODES)


def solution(mesh):
    in_specs = (P("feat", "rows"), P("rows"), P("rows", None), P("rows"), P("rows"))
    out_specs = (P("rows", "feat", None), P())
    group = mesh.shape["rows"]

    def step(*args):
        return on_device(group, mesh.shape["feat"], *args)

    return jax.shard_map(
        step, mesh=mesh, in_specs=in_specs, out_specs=out_specs, check_vma=False
    )
```

```python
import functools

import jax
import jax.numpy as jnp
from jax import lax
from jax.experimental import pallas as pl
from jax.experimental.pallas import tpu as pltpu
from jax.sharding import PartitionSpec as P


BINS = 256
FOLDS = 10
NODES = 4
PAIRS = FOLDS * NODES
COLS = 2 * PAIRS
TILE = 256
F8 = jnp.float8_e4m3fn
F32 = jnp.float32
BF16 = jnp.bfloat16


VMEM = pl.BlockSpec(memory_space=pltpu.VMEM)
SMEM = pl.BlockSpec(memory_space=pltpu.SMEM)
ANY = pl.BlockSpec(memory_space=pl.ANY)


def params():
    return pltpu.CompilerParams(vmem_limit_bytes=16 * 2**20)


def cost(flops, bytes_accessed=1 << 20):
    return pl.CostEstimate(
        flops=int(flops), bytes_accessed=int(bytes_accessed), transcendentals=0
    )


def weight_lines(low, high):
    shape = low.shape
    line = lax.broadcasted_iota(jnp.int32, shape, 0)
    node = (line % NODES).astype(F32)
    first = line < NODES
    fold = high[2:3]
    grads, hesss = [], []
    for j in range(FOLDS // 2):
        source, at = (low, 2 * j) if j < 4 else (high, 0)
        placed = jnp.where(first, source[at : at + 1], source[at + 1 : at + 2])
        k = jnp.where(first, F32(2 * j), F32(2 * j + 1))
        chosen = (placed == node) & (fold != k)
        grads.append(jnp.where(chosen, high[3:4], F32(0)))
        hesss.append(jnp.where(chosen, high[4:5], F32(0)))
    return jnp.concatenate(grads + hesss, axis=0).astype(BF16)


def one_hot(row, levels):
    packed = jnp.broadcast_to(row, (16, TILE)).astype(BF16)
    hit = jnp.concatenate([packed] * (BINS // 16), axis=0) == levels
    return jnp.where(hit, jnp.ones((), F8), jnp.zeros((), F8))


def bin_levels():
    return lax.broadcasted_iota(jnp.int32, (BINS, TILE), 0).astype(BF16)


def accumulate_pair(accs, feature, sources, levels):
    turn = 0
    for bins, line, weights, column, rows in sources:
        for at in range(0, rows, TILE):
            lhs = weights[:, pl.ds(column + at, TILE)]
            for q, acc in enumerate(accs):
                row = bins[pl.ds(line + feature + q, 1), pl.ds(at, TILE)]
                pltpu.matmul_push_rhs(
                    one_hot(row, levels), staging_register=turn % 2, mxu_index=q, transpose=True
                )
                pltpu.matmul_acc_lhs(acc, lhs, load_staged_rhs=turn % 2)
            turn += 1


def prepare_kernel(group, owned, size, me, parity, *refs):
    distant, refs = refs[:5], refs[5:]
    near, sems = refs[-6:-1], refs[-1]
    copies = [pltpu.make_async_copy(a, b, sems.at[i]) for i, (a, b) in enumerate(zip(distant, near))]
    for copy in copies:
        copy.start()
    bins, nodes, fold, gradient, hessian = near
    refs = refs[:-6]
    first, later = refs[: group - 1], refs[group - 1 : -2]
    own, rowdata = refs[-2:]
    rows = bins.shape[1]
    for copy in copies[1:]:
        copy.wait()
    rowdata[0:FOLDS] = nodes[...].astype(F32)
    rowdata[FOLDS + 3 :] = jnp.zeros((16 - FOLDS - 3, rows), F32)
    for i, ref in enumerate((fold, gradient, hessian)):
        lines = ref[...].astype(F32)
        for j in range(rows // 128):
            rowdata[FOLDS + i : FOLDS + i + 1, j * 128 : j * 128 + 128] = lines[j : j + 1]

    copies[0].wait()

    def move(to, at, source, count):
        if owned % 8 == 0:
            to[at : at + count] = bins[pl.ds(pl.multiple_of(source, 8), count)].astype(F32)
        else:
            for i in range(count):
                to[at + i : at + i + 1] = bins[pl.ds(source + i, 1)].astype(F32)

    for d in range(1, group):
        base = (me[0] ^ d) * owned
        first[d - 1][0:8] = rowdata[pl.ds(pl.multiple_of(parity[0] * 8, 8), 8)]
        move(first[d - 1], 8, base, size)
        if later:
            move(later[d - 1], 0, base + size, owned - size)
    move(own, 0, me[0] * owned, owned)


def prepare(me, parity, bins, nodes, fold, gradient, hessian, group, owned, size):
    rows = bins.shape[1]
    shapes = [(size + 8, rows)] * (group - 1)
    if owned > size:
        shapes += [(owned - size, rows)] * (group - 1)
    shapes += [(owned, rows), (16, rows)]
    wide = (rows // 128, 128)
    given = (bins, nodes.T, fold.reshape(wide), gradient.reshape(wide), hessian.reshape(wide))
    out = pl.pallas_call(
        functools.partial(prepare_kernel, group, owned, size),
        out_shape=[jax.ShapeDtypeStruct(shape, F32) for shape in shapes],
        in_specs=[SMEM, SMEM] + [pl.BlockSpec(memory_space=pltpu.HBM)] * 5,
        out_specs=[VMEM] * len(shapes),
        scratch_shapes=[pltpu.VMEM(x.shape, x.dtype) for x in given]
        + [pltpu.SemaphoreType.DMA((5,))],
        compiler_params=params(),
        cost_estimate=cost(1 << 30),
        name="prepare",
    )(me, parity, *given)
    return out[: group - 1], out[group - 1 : -2], out[-2], out[-1]


def own_kernel(bins, rowdata, *refs):
    outs, weights = refs[:-1], refs[-1]
    feats, rows = bins.shape
    size = feats // len(outs)

    def prepare(i, carry):
        at = pl.ds(pl.multiple_of(i * 512, 512), 512)
        weights[:, at] = weight_lines(rowdata[0:8, at], rowdata[8:16, at])
        return carry

    lax.fori_loop(0, rows // 512, prepare, 0)
    levels = bin_levels()

    def body(acc0, acc1):
        for c, out in enumerate(outs):

            def visit(p, carry, c=c, out=out):
                accumulate_pair((acc0, acc1), 2 * p, [(bins, c * size, weights, 0, rows)], levels)
                for q, acc in enumerate((acc0, acc1)):
                    at = pl.ds(pl.multiple_of((2 * p + q) * COLS, COLS), COLS)
                    out[at] = pltpu.matmul_pop(acc)
                return carry

            lax.fori_loop(0, size // 2, visit, 0, unroll=2 if size % 4 == 0 else 1)

    pl.run_scoped(body, pltpu.ACC(0)((COLS, BINS), F32), pltpu.ACC(1)((COLS, BINS), F32))


def own_part(bins, rowdata, size):
    feats, rows = bins.shape
    out = jax.ShapeDtypeStruct((size * COLS, BINS), F32)
    return pl.pallas_call(
        own_kernel,
        out_shape=[out] * (feats // size),
        in_specs=[VMEM, VMEM],
        out_specs=[VMEM] * (feats // size),
        scratch_shapes=[pltpu.VMEM((COLS, rows), BF16)],
        compiler_params=params(),
        cost_estimate=cost(2 * feats * rows * COLS * BINS),
        name="own_part",
    )(bins, rowdata)


def weights_kernel(count, rows, parity, *refs):
    mine, other, out = refs[:count], refs[count], refs[count + 1]
    even = parity[0] == 0
    for s in range(count):

        def prepare(i, carry, s=s):
            at = pl.ds(pl.multiple_of(i * 512, 512), 512)
            a = mine[s][0:8, at]
            b = other[8 * s : 8 * s + 8, at]
            to = pl.ds(pl.multiple_of(s * rows + i * 512, 512), 512)
            out[:, to] = weight_lines(jnp.where(even, a, b), jnp.where(even, b, a))
            return carry

        lax.fori_loop(0, rows // 512, prepare, 0)


def remote_weights(parity, mine, other):
    count = len(mine)
    rows = other.shape[1]
    return pl.pallas_call(
        functools.partial(weights_kernel, count, rows),
        out_shape=jax.ShapeDtypeStruct((COLS, count * rows), BF16),
        in_specs=[SMEM] + [VMEM] * (count + 1),
        out_specs=VMEM,
        compiler_params=params(),
        cost_estimate=cost(1 << 30),
        name="remote_weights",
    )(parity, *mine, other)


def chunk_kernel(count, group, line, feats, rows, final, waiting, me, part, best_in, weights, *refs):
    bins, ready, refs = refs[:count], refs[count : count + waiting], refs[count + waiting :]
    levels = bin_levels()
    sources = [(bins[s], line, weights, s * rows, rows) for s in range(count)]
    held = refs[-1]

    def body(acc0, acc1):
        accs = (acc0, acc1)

        def visit(p, carry):
            accumulate_pair(accs, 2 * p, sources, levels)
            for q, acc in enumerate(accs):
                at = pl.ds(pl.multiple_of((2 * p + q) * COLS, COLS), COLS)
                whole = pltpu.matmul_pop(acc) + part[at]
                for half in range(2):
                    held[half, at] = whole[:, half * 128 : half * 128 + 128]
            return carry

        lax.fori_loop(0, feats // 2, visit, 0)
        if not group:
            return
        lower = lax.broadcasted_iota(jnp.int32, (BINS, BINS), 0)
        upper = lax.broadcasted_iota(jnp.int32, (BINS, BINS), 1)
        triangle = (lower <= upper).astype(BF16)
        last = lax.broadcasted_iota(jnp.int32, (PAIRS, BINS), 1) == BINS - 1
        best = best_in[...]
        lists = [(ref, f) for ref in (*ready, held) for f in range(feats)]
        for p in range(0, len(lists), 2):
            for q, acc in enumerate(accs):
                ref, f = lists[p + q]
                if p == 0:
                    pltpu.matmul_push_rhs(triangle, staging_register=0, mxu_index=q)
                at = slice(f * COLS, (f + 1) * COLS)
                rest = jnp.concatenate([ref[0, at], ref[1, at]], axis=1)
                for piece in range(3):
                    high = rest.astype(BF16)
                    rest = rest - high.astype(F32)
                    pltpu.matmul_acc_lhs(
                        acc, high, load_staged_rhs=0 if p == 0 and piece == 0 else None
                    )
            for acc in accs:
                left = pltpu.matmul_pop(acc)
                gl, hl = left[:PAIRS], left[PAIRS:]
                g, h = gl[:, BINS - 1 :], hl[:, BINS - 1 :]
                gain = (
                    gl * gl / (hl + 1.0)
                    + (g - gl) * (g - gl) / (h - hl + 1.0)
                    - g * g / (h + 1.0)
                )
                best = jnp.maximum(best, jnp.where(last, F32(-3e38), gain))
        if final:
            best = jnp.broadcast_to(jnp.max(best, axis=1, keepdims=True), (PAIRS, 128))
        refs[group][...] = best

    pl.run_scoped(body, pltpu.ACC(0)((COLS, BINS), F32), pltpu.ACC(1)((COLS, BINS), F32))

    for d in range(group):
        share = COLS // group
        for j in range(share):
            row = (j % 2) * PAIRS + (me[0] ^ d) * (share // 2) + j // 2
            for half in range(2):
                lanes = slice(half * 128, half * 128 + 128)
                for c, ref in enumerate((*ready, held)):
                    refs[d][j, c * feats : (c + 1) * feats, lanes] = ref[
                        half, pl.ds(row, feats, stride=COLS), :
                    ]


def chunk(me, part, best, weights, bins, line, feats, group, final, ready):
    count = len(bins)
    rows = weights.shape[1] // count
    held = (2, feats * COLS, 128)
    if group:
        piece = (COLS // group, feats * (len(ready) + 1), BINS)
        shapes = [piece] * group + [(PAIRS, 128 if final else BINS)]
        scratch = [pltpu.VMEM(held, F32)]
    else:
        shapes, scratch = [held], []
    out = pl.pallas_call(
        functools.partial(chunk_kernel, count, group, line, feats, rows, final, len(ready)),
        out_shape=[jax.ShapeDtypeStruct(shape, F32) for shape in shapes],
        in_specs=[SMEM, VMEM, VMEM, VMEM] + [VMEM] * (count + len(ready)),
        out_specs=[VMEM] * len(shapes),
        scratch_shapes=scratch,
        compiler_params=params(),
        cost_estimate=cost(2 * feats * rows * count * COLS * BINS),
        name="chunk",
    )(me, part, best, weights, *bins, *ready)
    return out


def place_kernel(group, first, owned, feats, me, *refs):
    pieces, out, sems = refs[:group], refs[-2], refs[-1]
    copies = []
    for d in range(group):
        at = pl.multiple_of((me[0] ^ d) * owned + first, 8)
        copies.append(
            pltpu.make_async_copy(pieces[d], out.at[:, pl.ds(at, feats), :], sems.at[d])
        )
    for copy in copies:
        copy.start()
    for copy in copies:
        copy.wait()


def place(me, held, pieces, first, owned, shape):
    group = len(pieces)
    feats = pieces[0].shape[1]
    if owned % 8 or first % 8 or feats % 8:
        if held is None:
            held = jnp.zeros(shape, F32)
        for d, piece in enumerate(pieces):
            held = lax.dynamic_update_slice_in_dim(held, piece, (me[0] ^ d) * owned + first, 1)
        return held
    return pl.pallas_call(
        functools.partial(place_kernel, group, first, owned, feats),
        out_shape=jax.ShapeDtypeStruct(shape, F32),
        in_specs=[SMEM] + [VMEM] * group + ([] if held is None else [ANY]),
        out_specs=ANY,
        scratch_shapes=[pltpu.SemaphoreType.DMA((group,))],
        input_output_aliases={} if held is None else {group + 1: 0},
        compiler_params=params(),
        name="place",
    )(me, *pieces, *([] if held is None else [held]))


def on_device(group, feat_size, bins, fold, nodes, gradient, hessian):
    feats, _ = bins.shape
    owned = feats // group
    size = 8 if owned % 8 == 0 else owned
    chunks = owned // size
    me = lax.axis_index("rows")[None]
    parity = (lax.axis_index("feat") & 1)[None]
    others = range(1, group)

    def swap(x, axis, count, d):
        return lax.ppermute(x, axis, [(i, i ^ d) for i in range(count)])

    first, later, own, rowdata = prepare(
        me, parity, bins, nodes, fold, gradient, hessian, group, owned, size
    )
    arrived = [swap(first[d - 1], "rows", group, d) for d in others]
    if later:
        later = [swap(later[d - 1], "rows", group, d) for d in others]
    part = own_part(own, rowdata, size)
    traded = swap(jnp.concatenate([a[:8] for a in arrived]), "feat", feat_size, 1)
    weights = remote_weights(parity, arrived, traded)
    best = jnp.full((PAIRS, BINS), -3e38, F32)
    received, ready, began = [], [], 0
    for c in range(chunks):
        left = chunks - 1 - c
        send = left == 0 or left == 1
        source, line = (arrived, 8) if c == 0 else (later, (c - 1) * size)
        made = chunk(me, part[c], best, weights, source, line, size, group * send, left == 0, ready)
        if not send:
            ready = ready + list(made)
            continue
        best = made[-1]
        sent = [swap(made[d], "rows", group, d) for d in others]
        received.append((left, began, [made[0]] + sent))
        ready, began = [], (c + 1) * size
    step = 1
    while step < feat_size:
        best = jnp.maximum(best, swap(best, "feat", feat_size, step))
        step *= 2
    tops = [swap(best, "rows", group, d) for d in others]
    out = None
    for left, at, pieces in received:
        out = place(me, out, pieces, at, owned, (COLS // group, feats, BINS))
    for top in tops:
        best = jnp.maximum(best, top)
    return out, best[:, 0].reshape(FOLDS, NODES)


def solution(mesh):
    in_specs = (P("feat", "rows"), P("rows"), P("rows", None), P("rows"), P("rows"))
    out_specs = (P("rows", "feat", None), P())
    group = mesh.shape["rows"]

    def step(*args):
        return on_device(group, mesh.shape["feat"], *args)

    return jax.shard_map(
        step, mesh=mesh, in_specs=in_specs, out_specs=out_specs, check_vma=False
    )
```
